32 devices in a mesh: inst: 4 (over x, core), gx: 2 (over y), gy: 4 (over z).
Axes of the slice: x: 2, y: 2, z: 4, core: 2. Of those that a mesh axis runs over, the one named last changes fastest.
Arguments:
- state: float32 [8, 5, 16, 32, 128], P('inst', None, 'gx', 'gy'), may hold values from -6 to 6
- source: float32 [8, 5, 16, 32, 128], P('inst', None, 'gx', 'gy'), may hold values from -60 to 60
- jacobian: float32 [8, 5, 5, 16, 32, 128], P('inst', None, None, 'gx', 'gy'), may hold values from -1.5 to 16, as said below
- couplings: float32 [6, 5, 5], replicated, may hold values from -0.625 to 0.625
- omega: float32 [1], replicated, may hold values from 0.2 to 0.6
Outputs:
- state_next: float32 [8, 5, 16, 32, 128], P('inst', None, 'gx', 'gy')
- last_residual: float32 [8, 5, 16, 32, 128], P('inst', None, 'gx', 'gy')
The draws below stay inside these ranges and needn't reach their ends.
Inputs may be any that keep to these rules, and one draw needn't show every extreme that they name: In every block jacobian[n, :, :, cell] each diagonal entry lies in 8 to 16 and exceeds the sum of magnitudes of the other entries of its row by 2 or more.
All inputs are finite; a program needn't handle non-finite values.
Results may differ from the reference program's by a relative error of at most 0.0003.
Values sent between devices are 32-bit elements; how exact they have to be, the bound alone decides.
A program may use at most 64 MiB of HBM per device.

```python
import math
import jax
import jax.numpy as jnp
from jax import lax

NVAR = 5
NT = 8
ITERS = 3
NX = 16
NY = 32
NZ = 128


def draw_jacobian(key, part):
    first_key, second_key = jax.random.split(jax.random.fold_in(key, 17))
    shape = (NT, NVAR, NVAR, NX, NY, NZ)
    diagonal = jax.random.uniform(first_key, (NT, NVAR, NX, NY, NZ), jnp.float32, 8.0, 16.0)
    others = jnp.clip(0.6 * jax.random.normal(second_key, shape, jnp.float32), -1.5, 1.5)
    identity = jnp.eye(NVAR, dtype=jnp.float32)[None, :, :, None, None, None]
    return others * (1.0 - identity) + identity * diagonal[:, :, None]


def shard_levels(stream_key, shape, shards, least, largest):
    level, own = 1.0, jax.random.fold_in(stream_key, 6)
    for axis_at, blocks in shards:
        heights = jnp.exp(jax.random.uniform(jax.random.fold_in(own, axis_at), (blocks,), jnp.float32, least / len(shards), largest / len(shards)))
        level = level * jnp.repeat(heights, shape[axis_at] // blocks).reshape([-1 if axis == axis_at else 1 for axis in range(len(shape))])
    return level


def bell_draw(key, shape, scale, most, cuts=(), held_as=jnp.bfloat16):
    drawn = scale * jax.random.normal(key, shape, jnp.float32)
    if cuts:
        drawn = drawn * shard_levels(key, shape, cuts, -0.22, 0.18)
    return jnp.clip(drawn, -most, most).astype(held_as)


def setup_inputs(seed: int = 0) -> dict:
    streams_of = jax.random.split(jax.random.key(seed), 6)
    return {
        "state": bell_draw(streams_of[0], (NT, NVAR, NX, NY, NZ), 1.0, 6.0, ((0, 4), (2, 2), (3, 4)), jnp.float32),
        "source": bell_draw(streams_of[1], (NT, NVAR, NX, NY, NZ), 10.0, 60.0, ((0, 4), (2, 2), (3, 4)), jnp.float32),
        "jacobian": draw_jacobian(jax.random.fold_in(streams_of[5], 71), 0),
        "couplings": bell_draw(streams_of[3], (6, NVAR, NVAR), 100 ** -0.5, 0.625, (), jnp.float32),
        "omega": jnp.clip(jnp.exp(jax.random.uniform(streams_of[4], (1,), jnp.float32, math.log(0.2), math.log(0.6))), 0.2, 0.6),
    }


def spectral_table(row_index, column_index, total):
    offset = (row_index[:, None] - column_index[None, :]).astype(jnp.int32)
    parity = 1.0 - 2.0 * jnp.mod(offset, 2).astype(jnp.float32)
    angle = jnp.pi * offset.astype(jnp.float32) / total
    onsite = offset == 0
    sine = jnp.where(onsite, jnp.ones_like(angle), jnp.sin(angle))
    return jnp.where(onsite, jnp.zeros_like(angle), 0.5 * parity * jnp.cos(angle) / sine)


def pad_field(field):
    wrapped = jnp.concatenate([field[:, :, -1:], field, field[:, :, :1]], axis=2)
    return jnp.pad(wrapped, ((0, 0), (1, 1), (0, 0), (1, 1)))


def neighbours(padded, couplings):
    shifted = [padded[:, :-2, 1:-1, 1:-1], padded[:, 2:, 1:-1, 1:-1],
               padded[:, 1:-1, :-2, 1:-1], padded[:, 1:-1, 2:, 1:-1],
               padded[:, 1:-1, 1:-1, :-2], padded[:, 1:-1, 1:-1, 2:]]
    result = jnp.zeros(shifted[0].shape, jnp.float32)
    for direction in range(6):
        result = result + jnp.einsum("vw,wxyz->vxyz", couplings[direction], shifted[direction],
                                     precision=lax.Precision.HIGHEST)
    return result


def solve_blocks(blocks, right):
    size = blocks.shape[0]
    matrix = [[blocks[row, column] for column in range(size)] for row in range(size)]
    vector = [right[row] for row in range(size)]
    for pivot in range(size):
        for target in range(pivot + 1, size):
            factor = matrix[target][pivot] / matrix[pivot][pivot]
            for column in range(pivot + 1, size):
                matrix[target][column] = matrix[target][column] - factor * matrix[pivot][column]
            vector[target] = vector[target] - factor * vector[pivot]
    result = [None] * size
    for pivot in reversed(range(size)):
        total = vector[pivot]
        for column in range(pivot + 1, size):
            total = total - matrix[pivot][column] * result[column]
        result[pivot] = total / matrix[pivot][pivot]
    return jnp.stack(result, axis=0)


def reference(state, source, jacobian, couplings, omega):
    total = state.shape[0]
    positions = jnp.arange(total, dtype=jnp.int32)
    table = spectral_table(positions, positions, total)
    current = state
    residual = state
    for repeat in range(ITERS):
        spectral = omega[0] * jnp.einsum("nm,mvxyz->nvxyz", table, current,
                                         precision=lax.Precision.HIGHEST)

        def one_instance(pieces):
            field, blocks, right_side, spec_part = pieces
            beside = neighbours(pad_field(field), couplings)
            diagonal_part = jnp.einsum("vwxyz,wxyz->vxyz", blocks, field,
                                       precision=lax.Precision.HIGHEST)
            resid = right_side - diagonal_part - beside - spec_part
            return field + solve_blocks(blocks, resid), resid

        current, residual = lax.map(one_instance, (current, jacobian, source, spectral))
    return current, residual
```

```python
import functools
import math

import jax
import jax.numpy as jnp
from jax import lax
from jax.experimental import pallas as pl
from jax.experimental.pallas import tpu as pltpu
from jax.sharding import PartitionSpec as P

ITERS = 3
MESH = pl.DeviceIdType.MESH


def derivative(offset, total):
    offset = offset % total
    if offset > total // 2:
        offset -= total
    if offset == 0:
        return 0.0
    angle = math.pi * offset / total
    return 0.5 * (-1.0) ** offset * math.cos(angle) / math.sin(angle)


def factor(blocks):
    size = len(blocks)
    matrix = [list(row) for row in blocks]
    for pivot in range(size):
        matrix[pivot][pivot] = 1.0 / matrix[pivot][pivot]
        for target in range(pivot + 1, size):
            ratio = matrix[target][pivot] * matrix[pivot][pivot]
            matrix[target][pivot] = ratio
            for column in range(pivot + 1, size):
                matrix[target][column] = matrix[target][column] - ratio * matrix[pivot][column]
    return matrix


def substitute(matrix, right):
    size = len(right)
    vector = list(right)
    for pivot in range(size):
        for target in range(pivot + 1, size):
            vector[target] = vector[target] - matrix(target, pivot) * vector[pivot]
    result = [None] * size
    for pivot in reversed(range(size)):
        total = vector[pivot]
        for column in range(pivot + 1, size):
            total = total - matrix(pivot, column) * result[column]
        result[pivot] = total * matrix(pivot, pivot)
    return result


def weighted(weights, pieces):
    total = None
    for weight, piece in zip(weights, pieces):
        if isinstance(weight, float) and weight == 0.0:
            continue
        term = weight * piece
        total = term if total is None else total + term
    return total


def kernel(
    ranks, count_x, count_y,
    state, source, jacobian, couplings, omega,
    state_next, last_residual,
    cur, peer, part, got, low_out, high_out, low_in, high_in,
    rhs, blocks, lu, final, resid,
    load_sem, peer_send, peer_recv, part_send, part_recv,
    edge_send, edge_recv, side_send, side_recv, store_sem,
):
    local, nvar, planes, rows, depth = state.shape
    total = local * ranks
    pairs = ranks // 2
    rank = lax.axis_index("inst")
    at_x = lax.axis_index("gx")
    at_y = lax.axis_index("gy")
    pair = rank // 2
    core = rank % 2
    partner = pair * 2 + 1 - core
    up = (at_y + 1) % count_y
    down = (at_y + count_y - 1) % count_y
    has_low = at_x > 0
    has_high = at_x < count_x - 1
    flip = at_x % 2 == 0

    def plane_of(step):
        return jnp.where(flip, planes - 1 - step, step)

    def load_state(x):
        return pltpu.make_async_copy(state.at[:, :, x], cur.at[0, x + 1], load_sem.at[0, x])

    def load_source(x):
        return pltpu.make_async_copy(source.at[:, :, x], rhs.at[x], load_sem.at[1, x])

    def load_blocks(x):
        return pltpu.make_async_copy(jacobian.at[:, :, :, x], blocks.at[x], load_sem.at[2, x])

    def store_state(x):
        return pltpu.make_async_copy(final.at[x], state_next.at[:, :, x], store_sem.at[0, x])

    def store_resid(x):
        return pltpu.make_async_copy(resid.at[x], last_residual.at[:, :, x], store_sem.at[1, x])

    def to_peer(k, x):
        return pltpu.make_async_remote_copy(
            cur.at[k, x + 1], peer.at[k, x], peer_send.at[k, x], peer_recv.at[k, x],
            device_id={"inst": partner}, device_id_type=MESH)

    def to_pair(k, x, hop):
        target = ((pair + hop) % pairs) * 2 + core
        return pltpu.make_async_remote_copy(
            part.at[k, hop - 1, x], got.at[k, hop - 1, x],
            part_send.at[k, hop - 1, x], part_recv.at[k, hop - 1, x],
            device_id={"inst": target}, device_id_type=MESH)

    def to_up(k, x):
        return pltpu.make_async_remote_copy(
            high_out.at[k, x], low_in.at[k, x], edge_send.at[0, k, x], edge_recv.at[0, k, x],
            device_id={"gy": up}, device_id_type=MESH)

    def to_down(k, x):
        return pltpu.make_async_remote_copy(
            low_out.at[k, x], high_in.at[k, x], edge_send.at[1, k, x], edge_recv.at[1, k, x],
            device_id={"gy": down}, device_id_type=MESH)

    def to_next(k):
        return pltpu.make_async_remote_copy(
            cur.at[k, planes], cur.at[k, 0], side_send.at[0, k], side_recv.at[0, k],
            device_id={"gx": at_x + 1}, device_id_type=MESH)

    def to_last(k):
        return pltpu.make_async_remote_copy(
            cur.at[k, 1], cur.at[k, planes + 1], side_send.at[1, k], side_recv.at[1, k],
            device_id={"gx": at_x - 1}, device_id_type=MESH)

    def send_planes(k, x):
        to_peer(k, x).start()

        @pl.when(jnp.logical_and(x == planes - 1, has_high))
        def _():
            to_next(k).start()

        @pl.when(jnp.logical_and(x == 0, has_low))
        def _():
            to_last(k).start()

    def send_edges(k, x, field):
        for n in range(local):
            for v in range(nvar):
                at = n * nvar + v
                low_out[k, x, at:at + 1] = field[n][v][:1]
                high_out[k, x, at:at + 1] = field[n][v][rows - 1:]

    def start_edges(k, x):
        to_up(k, x).start()
        to_down(k, x).start()

    def mine(k, x):
        return [[cur[k, x + 1, n, v] for v in range(nvar)] for n in range(local)]

    even = core == 0

    def weights_of(hop, a):
        own = [derivative(2 * local * hop + a - b, total) for b in range(local)]
        other = [
            jnp.where(
                even,
                jnp.float32(derivative(2 * local * hop - local + a - b, total)),
                jnp.float32(derivative(2 * local * hop + local + a - b, total)),
            )
            for b in range(local)
        ]
        return own + other

    def send_parts(k, x):
        to_peer(k, x).wait_recv()
        for hop in range(1, pairs):
            for a in range(local):
                weights = weights_of(hop, a)
                for v in range(nvar):
                    pieces = [cur[k, x + 1, b, v] for b in range(local)]
                    pieces += [peer[k, x, b, v] for b in range(local)]
                    part[k, hop - 1, x, a, v] = weighted(weights, pieces)
            to_pair(k, x, hop).start()

    for step in range(planes):
        load_state(plane_of(step)).start()
    for step in range(planes):
        load_blocks(plane_of(step)).start()
        load_source(plane_of(step)).start()

    barrier = pltpu.get_barrier_semaphore()

    def greet(**where):
        pl.semaphore_signal(barrier, inc=1, device_id=where, device_id_type=MESH)

    greet(inst=partner)
    for hop in range(1, pairs):
        greet(inst=((pair + hop) % pairs) * 2 + core)
    greet(gy=up)
    greet(gy=down)

    @pl.when(has_low)
    def _():
        greet(gx=at_x - 1)

    @pl.when(has_high)
    def _():
        greet(gx=at_x + 1)

    zero = jnp.zeros((local, nvar, rows, depth), jnp.float32)

    @pl.when(jnp.logical_not(has_low))
    def _():
        for k in range(ITERS):
            cur[k, 0] = zero

    @pl.when(jnp.logical_not(has_high))
    def _():
        for k in range(ITERS):
            cur[k, planes + 1] = zero

    sides = has_low.astype(jnp.int32) + has_high.astype(jnp.int32)
    pl.semaphore_wait(barrier, pairs + 2 + sides)

    @pl.loop(0, planes)
    def _(step):
        x = plane_of(step)
        load_state(x).wait()
        send_planes(0, x)

    @pl.loop(0, planes)
    def _(step):
        send_parts(0, plane_of(step))

    @pl.loop(0, planes)
    def _(step):
        x = plane_of(step)
        send_edges(0, x, mine(0, x))
        start_edges(0, x)

    row_at = lax.broadcasted_iota(jnp.int32, (rows, depth), 0)
    lane_at = lax.broadcasted_iota(jnp.int32, (rows, depth), 1)
    first_row, final_row = row_at == 0, row_at == rows - 1
    first_lane, final_lane = lane_at == 0, lane_at == depth - 1
    speed = omega[0]

    def right_side(k, x, n):
        result = []
        for v in range(nvar):
            result.append(None)
        for w in range(nvar):
            field = cur[k, x + 1, n, w]
            at = n * nvar + w
            shifted = [
                cur[k, x, n, w],
                cur[k, x + 2, n, w],
                jnp.where(first_row, low_in[k, x, at:at + 1], pltpu.roll(field, 1, 0)),
                jnp.where(final_row, high_in[k, x, at:at + 1], pltpu.roll(field, rows - 1, 0)),
                jnp.where(first_lane, 0.0, pltpu.roll(field, 1, 1)),
                jnp.where(final_lane, 0.0, pltpu.roll(field, depth - 1, 1)),
            ]
            for v in range(nvar):
                term = weighted([couplings[v, d, w] for d in range(6)], shifted)
                result[v] = term if result[v] is None else result[v] + term
        weights = weights_of(0, n)
        for v in range(nvar):
            pieces = [cur[k, x + 1, b, v] for b in range(local)]
            pieces += [peer[k, x, b, v] for b in range(local)]
            spectral = weighted(weights, pieces)
            for hop in range(1, pairs):
                spectral = spectral + got[k, hop - 1, x, n, v]
            result[v] = rhs[x, n, v] - result[v] - speed * spectral
        return result

    for k in range(ITERS):
        final_pass = k == ITERS - 1

        @pl.loop(0, planes)
        def _(step, k=k, final_pass=final_pass):
            x = plane_of(step)
            if k == 0:
                load_blocks(x).wait()
                for n in range(local):
                    matrix = factor(
                        [[blocks[x, n, v, w] for w in range(nvar)] for v in range(nvar)])
                    for v in range(nvar):
                        for w in range(nvar):
                            lu[x, n, v, w] = matrix[v][w]
                load_source(x).wait()

            @pl.when(jnp.logical_and(x == 0, has_low))
            def _():
                to_next(k).wait_recv()

            @pl.when(jnp.logical_and(x == planes - 1, has_high))
            def _():
                to_last(k).wait_recv()

            to_up(k, x).wait_recv()
            to_down(k, x).wait_recv()
            for hop in range(1, pairs):
                to_pair(k, x, hop).wait_recv()
            fields = []
            for n in range(local):
                right = right_side(k, x, n)
                if final_pass:
                    own = [cur[k, x + 1, n, w] for w in range(nvar)]
                    for v in range(nvar):
                        for w in range(nvar):
                            right[v] = right[v] - blocks[x, n, v, w] * own[w]
                        resid[x, n, v] = right[v]
                answer = substitute(lambda v, w: lu[x, n, v, w], right)
                if final_pass:
                    for v in range(nvar):
                        final[x, n, v] = own[v] + answer[v]
                else:
                    for v in range(nvar):
                        cur[k + 1, x + 1, n, v] = answer[v]
                    fields.append(answer)
            if final_pass:
                store_resid(x).start()
                store_state(x).start()
            else:
                send_edges(k + 1, x, fields)
                send_planes(k + 1, x)
                start_edges(k + 1, x)

                @pl.when(step > 0)
                def _():
                    send_parts(k + 1, plane_of(step - 1))

            if k > 0:

                @pl.when(step == 0)
                def _():
                    send_parts(k, plane_of(planes - 1))

    @pl.loop(0, planes)
    def _(x):
        for k in range(ITERS):
            to_peer(k, x).wait_send()
            for hop in range(1, pairs):
                to_pair(k, x, hop).wait_send()
            to_up(k, x).wait_send()
            to_down(k, x).wait_send()
        store_resid(x).wait()
        store_state(x).wait()

    for k in range(ITERS):

        @pl.when(has_high)
        def _():
            to_next(k).wait_send()

        @pl.when(has_low)
        def _():
            to_last(k).wait_send()


def solution(mesh):
    ranks, count_x, count_y = mesh.shape["inst"], mesh.shape["gx"], mesh.shape["gy"]

    def shards(state, source, jacobian, couplings, omega):
        local, nvar, planes, rows, depth = state.shape
        pairs = ranks // 2
        cell = (local, nvar, rows, depth)
        edge = pltpu.VMEM((ITERS, planes, local * nvar, depth), jnp.float32)
        hbm = pl.BlockSpec(memory_space=pl.ANY)
        smem = pl.BlockSpec(memory_space=pltpu.SMEM)
        dma = pltpu.SemaphoreType.DMA
        vmem = lambda *lead: pltpu.VMEM(lead + cell, jnp.float32)
        matrices = pltpu.VMEM((planes, local, nvar, nvar, rows, depth), jnp.float32)
        return tuple(pl.pallas_call(
            functools.partial(kernel, ranks, count_x, count_y),
            out_shape=[jax.ShapeDtypeStruct(state.shape, jnp.float32)] * 2,
            in_specs=[hbm, hbm, hbm, smem, smem],
            out_specs=[hbm, hbm],
            scratch_shapes=[
                vmem(ITERS, planes + 2), vmem(ITERS, planes),
                vmem(ITERS, pairs - 1, planes), vmem(ITERS, pairs - 1, planes),
                edge, edge, edge, edge,
                vmem(planes), matrices, matrices, vmem(planes), vmem(planes),
                dma((3, planes)), dma((ITERS, planes)), dma((ITERS, planes)),
                dma((ITERS, pairs - 1, planes)), dma((ITERS, pairs - 1, planes)),
                dma((2, ITERS, planes)), dma((2, ITERS, planes)),
                dma((2, ITERS)), dma((2, ITERS)), dma((2, planes)),
            ],
            compiler_params=pltpu.CompilerParams(
                collective_id=0, has_side_effects=True, vmem_limit_bytes=48 * 2**20),
            name="smooth",
        )(state, source, jacobian, couplings.transpose(1, 0, 2), omega))

    split = P("inst", None, "gx", "gy", None)
    return jax.shard_map(
        shards,
        mesh=mesh,
        in_specs=(split, split, P("inst", None, None, "gx", "gy", None), P(), P()),
        out_specs=(split, split),
        check_vma=False,
    )
```

```python
import functools
import math

import jax
import jax.numpy as jnp
from jax import lax
from jax.experimental import pallas as pl
from jax.experimental.pallas import tpu as pltpu
from jax.sharding import PartitionSpec as P

ITERS = 3
LAG = 2
MESH = pl.DeviceIdType.MESH


def derivative(offset, total):
    offset = offset % total
    if offset > total // 2:
        offset -= total
    if offset == 0:
        return 0.0
    angle = math.pi * offset / total
    return 0.5 * (-1.0) ** offset * math.cos(angle) / math.sin(angle)


def factor(blocks):
    size = len(blocks)
    matrix = [list(row) for row in blocks]
    for pivot in range(size):
        matrix[pivot][pivot] = 1.0 / matrix[pivot][pivot]
        for target in range(pivot + 1, size):
            ratio = matrix[target][pivot] * matrix[pivot][pivot]
            matrix[target][pivot] = ratio
            for column in range(pivot + 1, size):
                matrix[target][column] = matrix[target][column] - ratio * matrix[pivot][column]
    return matrix


def substitute(matrix, right):
    size = len(right)
    vector = list(right)
    for pivot in range(size):
        for target in range(pivot + 1, size):
            vector[target] = vector[target] - matrix(target, pivot) * vector[pivot]
    result = [None] * size
    for pivot in reversed(range(size)):
        total = vector[pivot]
        for column in range(pivot + 1, size):
            total = total - matrix(pivot, column) * result[column]
        result[pivot] = total * matrix(pivot, pivot)
    return result


def weighted(weights, pieces):
    total = None
    for weight, piece in zip(weights, pieces):
        if isinstance(weight, float) and weight == 0.0:
            continue
        term = weight * piece
        total = term if total is None else total + term
    return total


def kernel(
    ranks, count_x, count_y,
    state, source, jacobian, couplings, omega,
    state_next, last_residual,
    cur, peer, part, got, low_out, high_out, low_in, high_in,
    rhs, blocks, lu, final, resid,
    load_sem, peer_send, peer_recv, part_send, part_recv,
    edge_send, edge_recv, side_send, side_recv, store_sem,
):
    local, nvar, planes, rows, depth = state.shape
    total = local * ranks
    pairs = ranks // 2
    rank = lax.axis_index("inst")
    at_x = lax.axis_index("gx")
    at_y = lax.axis_index("gy")
    pair = rank // 2
    core = rank % 2
    partner = pair * 2 + 1 - core
    up = (at_y + 1) % count_y
    down = (at_y + count_y - 1) % count_y
    has_low = at_x > 0
    has_high = at_x < count_x - 1
    flip = at_x % 2 == 0

    def plane_of(step):
        return jnp.where(flip, planes - 1 - step, step)

    def load_state(x):
        return pltpu.make_async_copy(state.at[:, :, x], cur.at[0, x + 1], load_sem.at[0, x])

    def load_source(x):
        return pltpu.make_async_copy(source.at[:, :, x], rhs.at[x], load_sem.at[1, x])

    def load_blocks(x):
        return pltpu.make_async_copy(jacobian.at[:, :, :, x], blocks.at[x], load_sem.at[2, x])

    def store_state(x):
        return pltpu.make_async_copy(final.at[x], state_next.at[:, :, x], store_sem.at[0, x])

    def store_resid(x):
        return pltpu.make_async_copy(resid.at[x], last_residual.at[:, :, x], store_sem.at[1, x])

    def to_peer(k, x):
        return pltpu.make_async_remote_copy(
            cur.at[k, x + 1], peer.at[k, x], peer_send.at[k, x], peer_recv.at[k, x],
            device_id={"inst": partner}, device_id_type=MESH)

    def to_pair(k, x, hop):
        target = ((pair + hop) % pairs) * 2 + core
        return pltpu.make_async_remote_copy(
            part.at[k, hop - 1, x], got.at[k, hop - 1, x],
            part_send.at[k, hop - 1, x], part_recv.at[k, hop - 1, x],
            device_id={"inst": target}, device_id_type=MESH)

    def to_up(k, x):
        return pltpu.make_async_remote_copy(
            high_out.at[k, x], low_in.at[k, x], edge_send.at[0, k, x], edge_recv.at[0, k, x],
            device_id={"gy": up}, device_id_type=MESH)

    def to_down(k, x):
        return pltpu.make_async_remote_copy(
            low_out.at[k, x], high_in.at[k, x], edge_send.at[1, k, x], edge_recv.at[1, k, x],
            device_id={"gy": down}, device_id_type=MESH)

    def to_next(k):
        return pltpu.make_async_remote_copy(
            cur.at[k, planes], cur.at[k, 0], side_send.at[0, k], side_recv.at[0, k],
            device_id={"gx": at_x + 1}, device_id_type=MESH)

    def to_last(k):
        return pltpu.make_async_remote_copy(
            cur.at[k, 1], cur.at[k, planes + 1], side_send.at[1, k], side_recv.at[1, k],
            device_id={"gx": at_x - 1}, device_id_type=MESH)

    def send_planes(k, x):
        to_peer(k, x).start()

        @pl.when(jnp.logical_and(x == planes - 1, has_high))
        def _():
            to_next(k).start()

        @pl.when(jnp.logical_and(x == 0, has_low))
        def _():
            to_last(k).start()

    def send_edges(k, x, field):
        for n in range(local):
            for v in range(nvar):
                at = n * nvar + v
                low_out[k, x, at:at + 1] = field[n][v][:1]
                high_out[k, x, at:at + 1] = field[n][v][rows - 1:]

    def start_edges(k, x):
        to_up(k, x).start()
        to_down(k, x).start()

    def mine(k, x):
        return [[cur[k, x + 1, n, v] for v in range(nvar)] for n in range(local)]

    even = core == 0

    def weights_of(hop, a):
        own = [derivative(2 * local * hop + a - b, total) for b in range(local)]
        other = [
            jnp.where(
                even,
                jnp.float32(derivative(2 * local * hop - local + a - b, total)),
                jnp.float32(derivative(2 * local * hop + local + a - b, total)),
            )
            for b in range(local)
        ]
        return own + other

    def send_parts(k, x):
        to_peer(k, x).wait_recv()
        for hop in range(1, pairs):
            for a in range(local):
                weights = weights_of(hop, a)
                for v in range(nvar):
                    pieces = [cur[k, x + 1, b, v] for b in range(local)]
                    pieces += [peer[k, x, b, v] for b in range(local)]
                    part[k, hop - 1, x, a, v] = weighted(weights, pieces)
            to_pair(k, x, hop).start()

    for step in range(planes):
        load_state(plane_of(step)).start()
    for step in range(planes):
        load_blocks(plane_of(step)).start()
        load_source(plane_of(step)).start()

    barrier = pltpu.get_barrier_semaphore()

    def greet(**where):
        pl.semaphore_signal(barrier, inc=1, device_id=where, device_id_type=MESH)

    greet(inst=partner)
    for hop in range(1, pairs):
        greet(inst=((pair + hop) % pairs) * 2 + core)
    greet(gy=up)
    greet(gy=down)

    @pl.when(has_low)
    def _():
        greet(gx=at_x - 1)

    @pl.when(has_high)
    def _():
        greet(gx=at_x + 1)

    zero = jnp.zeros((local, nvar, rows, depth), jnp.float32)

    @pl.when(jnp.logical_not(has_low))
    def _():
        for k in range(ITERS):
            cur[k, 0] = zero

    @pl.when(jnp.logical_not(has_high))
    def _():
        for k in range(ITERS):
            cur[k, planes + 1] = zero

    sides = has_low.astype(jnp.int32) + has_high.astype(jnp.int32)
    pl.semaphore_wait(barrier, pairs + 2 + sides)

    @pl.loop(0, planes)
    def _(step):
        x = plane_of(step)
        load_state(x).wait()
        send_planes(0, x)

    @pl.loop(0, planes)
    def _(step):
        send_parts(0, plane_of(step))

    @pl.loop(0, planes)
    def _(step):
        x = plane_of(step)
        send_edges(0, x, mine(0, x))
        start_edges(0, x)

    row_at = lax.broadcasted_iota(jnp.int32, (rows, depth), 0)
    lane_at = lax.broadcasted_iota(jnp.int32, (rows, depth), 1)
    first_row, final_row = row_at == 0, row_at == rows - 1
    first_lane, final_lane = lane_at == 0, lane_at == depth - 1
    speed = omega[0]
    lag = min(LAG, planes)

    def right_side(k, x, n):
        result = []
        for v in range(nvar):
            result.append(None)
        for w in range(nvar):
            field = cur[k, x + 1, n, w]
            at = n * nvar + w
            shifted = [
                cur[k, x, n, w],
                cur[k, x + 2, n, w],
                jnp.where(first_row, low_in[k, x, at:at + 1], pltpu.roll(field, 1, 0)),
                jnp.where(final_row, high_in[k, x, at:at + 1], pltpu.roll(field, rows - 1, 0)),
                jnp.where(first_lane, 0.0, pltpu.roll(field, 1, 1)),
                jnp.where(final_lane, 0.0, pltpu.roll(field, depth - 1, 1)),
            ]
            for v in range(nvar):
                term = weighted([couplings[v, d, w] for d in range(6)], shifted)
                result[v] = term if result[v] is None else result[v] + term
        weights = weights_of(0, n)
        for v in range(nvar):
            pieces = [cur[k, x + 1, b, v] for b in range(local)]
            pieces += [peer[k, x, b, v] for b in range(local)]
            spectral = weighted(weights, pieces)
            for hop in range(1, pairs):
                spectral = spectral + got[k, hop - 1, x, n, v]
            result[v] = rhs[x, n, v] - result[v] - speed * spectral
        return result

    for k in range(ITERS):
        final_pass = k == ITERS - 1

        @pl.loop(0, planes)
        def _(step, k=k, final_pass=final_pass):
            x = plane_of(step)
            if k == 0:
                load_blocks(x).wait()
                for n in range(local):
                    matrix = factor(
                        [[blocks[x, n, v, w] for w in range(nvar)] for v in range(nvar)])
                    for v in range(nvar):
                        for w in range(nvar):
                            lu[x, n, v, w] = matrix[v][w]
                load_source(x).wait()

            @pl.when(jnp.logical_and(x == 0, has_low))
            def _():
                to_next(k).wait_recv()

            @pl.when(jnp.logical_and(x == planes - 1, has_high))
            def _():
                to_last(k).wait_recv()

            to_up(k, x).wait_recv()
            to_down(k, x).wait_recv()
            for hop in range(1, pairs):
                to_pair(k, x, hop).wait_recv()
            fields = []
            for n in range(local):
                right = right_side(k, x, n)
                if final_pass:
                    own = [cur[k, x + 1, n, w] for w in range(nvar)]
                    for v in range(nvar):
                        for w in range(nvar):
                            right[v] = right[v] - blocks[x, n, v, w] * own[w]
                        resid[x, n, v] = right[v]
                answer = substitute(lambda v, w: lu[x, n, v, w], right)
                if final_pass:
                    for v in range(nvar):
                        final[x, n, v] = own[v] + answer[v]
                else:
                    for v in range(nvar):
                        cur[k + 1, x + 1, n, v] = answer[v]
                    fields.append(answer)
            if final_pass:
                store_resid(x).start()
                store_state(x).start()
            else:
                send_edges(k + 1, x, fields)
                send_planes(k + 1, x)
                start_edges(k + 1, x)

                @pl.when(step >= lag)
                def _():
                    send_parts(k + 1, plane_of(step - lag))

            if k > 0:

                @pl.when(step < lag)
                def _():
                    send_parts(k, plane_of(planes - lag + step))

    @pl.loop(0, planes)
    def _(x):
        for k in range(ITERS):
            to_peer(k, x).wait_send()
            for hop in range(1, pairs):
                to_pair(k, x, hop).wait_send()
            to_up(k, x).wait_send()
            to_down(k, x).wait_send()
        store_resid(x).wait()
        store_state(x).wait()

    for k in range(ITERS):

        @pl.when(has_high)
        def _():
            to_next(k).wait_send()

        @pl.when(has_low)
        def _():
            to_last(k).wait_send()


def solution(mesh):
    ranks, count_x, count_y = mesh.shape["inst"], mesh.shape["gx"], mesh.shape["gy"]

    def shards(state, source, jacobian, couplings, omega):
        local, nvar, planes, rows, depth = state.shape
        pairs = ranks // 2
        cell = (local, nvar, rows, depth)
        edge = pltpu.VMEM((ITERS, planes, local * nvar, depth), jnp.float32)
        hbm = pl.BlockSpec(memory_space=pl.ANY)
        smem = pl.BlockSpec(memory_space=pltpu.SMEM)
        dma = pltpu.SemaphoreType.DMA
        vmem = lambda *lead: pltpu.VMEM(lead + cell, jnp.float32)
        matrices = pltpu.VMEM((planes, local, nvar, nvar, rows, depth), jnp.float32)
        return tuple(pl.pallas_call(
            functools.partial(kernel, ranks, count_x, count_y),
            out_shape=[jax.ShapeDtypeStruct(state.shape, jnp.float32)] * 2,
            in_specs=[hbm, hbm, hbm, smem, smem],
            out_specs=[hbm, hbm],
            scratch_shapes=[
                vmem(ITERS, planes + 2), vmem(ITERS, planes),
                vmem(ITERS, pairs - 1, planes), vmem(ITERS, pairs - 1, planes),
                edge, edge, edge, edge,
                vmem(planes), matrices, matrices, vmem(planes), vmem(planes),
                dma((3, planes)), dma((ITERS, planes)), dma((ITERS, planes)),
                dma((ITERS, pairs - 1, planes)), dma((ITERS, pairs - 1, planes)),
                dma((2, ITERS, planes)), dma((2, ITERS, planes)),
                dma((2, ITERS)), dma((2, ITERS)), dma((2, planes)),
            ],
            compiler_params=pltpu.CompilerParams(
                collective_id=0, has_side_effects=True, vmem_limit_bytes=60 * 1024 * 1024),
            name="smooth",
        )(state, source, jacobian, couplings.transpose(1, 0, 2), omega))

    split = P("inst", None, "gx", "gy", None)
    return jax.shard_map(
        shards,
        mesh=mesh,
        in_specs=(split, split, P("inst", None, None, "gx", "gy", None), P(), P()),
        out_specs=(split, split),
        check_vma=False,
    )
```
